32 devices in a mesh: gx: 2 (over x), gy: 4 (over y, core), gz: 4 (over z).
Axes of the slice: x: 2, y: 2, z: 4, core: 2. Of those that a mesh axis runs over, the one named last changes fastest.
Arguments:
- blocks: bfloat16 [512, 128, 1024], P(('gx', 'gy', 'gz')), may hold values from -0.375 to 0.375
- counts: int32 [512], P(('gx', 'gy', 'gz')), may hold values from 1 to 128
- owner: int32 [512, 1], P(('gx', 'gy', 'gz')), may hold values from 0 to 15; in each aligned block of 16 rows (0 to 15, 16 to 31, ...) no two rows name the same one
- kdiag: float32 [32, 1024], P(('gx', 'gy', 'gz')), may hold values from 0.5 to 4
- rhs: float32 [32, 1024], P(('gx', 'gy', 'gz')), may hold values from -40 to 40
- modes: float32 [32, 6, 1024], P(('gx', 'gy', 'gz')), may hold values from -6 to 6
Outputs:
- schur: bfloat16 [32, 1024, 1024], P(('gx', 'gy', 'gz'))
- solution: float32 [32, 1024], P(('gx', 'gy', 'gz'))
- residual: float32 [32, 1024], P(('gx', 'gy', 'gz'))
The draws below stay inside these ranges and needn't reach their ends.
Inputs may be any that keep to these rules, and one draw needn't show every extreme that they name: `owner`: the 16 blocks of one device go to different owners.
All inputs are finite; a program needn't handle non-finite values.
Results may differ from the reference program's by a relative error of at most 0.001.
Values may be sent and summed in bfloat16 or wider, within the bound.
A program may use at most 64 MiB of HBM per device.

```python
import math
import jax
import jax.numpy as jnp
import numpy as np
from jax import lax

NB = 1024
ROWS = 128
BLK_DEV = 16
NC = 6
ITERS = 2
SUBDOMAINS = 32
BLOCKS = 512
N_GX = 2
N_GY = 4
N_GZ = 4


def draw_rhs(key, part):
    index = jnp.arange(SUBDOMAINS, dtype=jnp.float32)[:, None]
    scale = 4.0 * (1.0 + 2.0 * index / max(SUBDOMAINS - 1, 1))
    values = jax.random.normal(jax.random.fold_in(key, 11), (SUBDOMAINS, NB), jnp.float32) * scale
    return jnp.clip(values, -40.0, 40.0)


def touch_ends(values, own_key, least, high):
    shape = values.shape
    place = [jax.random.randint(jax.random.fold_in(own_key, axis), (), 0, shape[axis]) for axis in range(len(shape))]
    values = values.at[tuple(place)].set(least)
    longest = shape.index(max(shape))
    place[longest] = (place[longest] + 1) % shape[longest]
    return values.at[tuple(place)].set(high)


def levels(rng, dims, cuts, low, top_value):
    def one(axis_at, parts):
        heights = jax.random.uniform(jax.random.fold_in(jax.random.fold_in(rng, 6), axis_at), (parts,), jnp.float32, low / len(cuts), top_value / len(cuts))
        return jnp.repeat(jnp.exp(heights), dims[axis_at] // parts).reshape((-1,) + (1,) * (len(dims) - axis_at - 1))

    factor_of = one(*cuts[0])
    for cut in cuts[1:]:
        factor_of = factor_of * one(*cut)
    return factor_of


def assign_block(stream_key, own, number, rows, count, top, limit, lean):
    ranking = jax.random.permutation(stream_key, count)
    crowded, ordinary = load_shares(count, rows * top, limit, lean, True), load_shares(count, rows * top, limit, lean, False)
    places = jnp.arange(count)

    def named(tallies, offset_by):
        used = int((tallies > 0).sum())
        fixed = max(1, used // 4)
        moved = fixed + (places - fixed + offset_by * (used - fixed)) % max(1, count - fixed)
        return jnp.zeros((count,), jnp.int32).at[ranking[jnp.where(places < fixed, places, moved)]].set(jnp.asarray(tallies, jnp.int32))

    tallies = jnp.where(number % 4 == 0, named(crowded, number // 4), named(ordinary, number - number // 4 - 1))
    mixed = jax.random.permutation(jax.random.fold_in(own, 3), count)
    donor, receiver = mixed[0:count // 2 * 2:2], mixed[1:count // 2 * 2:2]
    room = jnp.minimum(tallies[donor] - 1, limit - tallies[receiver]) // 2
    room = jnp.where((donor == ranking[0]) | (receiver == ranking[0]) | (tallies[receiver] == 0), 0, jnp.maximum(room, 0))
    moved = jax.random.randint(jax.random.fold_in(own, 4), (count // 2,), 0, 1 << 20) % (room + 1)
    tallies = tallies.at[donor].add(-moved).at[receiver].add(moved)
    labels = jnp.searchsorted(jnp.cumsum(tallies), jnp.arange(rows * top), side="right").astype(jnp.int32)
    table = labels.reshape(top, rows).T
    table = table[jax.random.permutation(jax.random.fold_in(own, 1), rows)]
    offset_by = jax.random.randint(jax.random.fold_in(own, 2), (rows, 1), 0, top)
    return jnp.take_along_axis(table, (jnp.arange(top)[None, :] + offset_by) % top, axis=1)


def load_shares(count, total, bound, slope, full):
    portions = [(1 << 20) // math.isqrt(rank ** slope) + 1 for rank in range(1, count + 1)]
    largest = bound if full else min(bound, max(-(-total // count), total * portions[0] // sum(portions)))
    least = 1 if total - largest >= count - 1 else 0
    given, surplus = [largest] + [least] * (count - 1), total - largest - least * (count - 1)
    while surplus > 0:
        free = [i for i in range(1, count) if given[i] < largest] or [i for i in range(1, count) if given[i] < bound]
        pool, left = sum([portions[i] for i in free]), surplus
        for i in free:
            more = min(bound - given[i], max(1, left * portions[i] // pool), surplus)
            given[i] = given[i] + more
            surplus = surplus - more
    return np.array(given)


def noise(key, extent, scale, reach, cuts=(), kind=jnp.bfloat16):
    loudness = levels(key, extent, cuts, -0.22, 0.18) if cuts else 1.0
    array = jax.random.normal(key, extent, jnp.float32) * scale * loudness
    return jnp.minimum(jnp.maximum(array, -reach), reach).astype(kind)


def setup_inputs(seed: int = 0) -> dict:
    key_of = jax.random.split(jax.random.key(seed), 7)
    blocks = noise(key_of[0], (BLOCKS, ROWS, NB), 0.0625, 0.375, ((0, 32),))
    counts = touch_ends(jax.random.randint(key_of[1], (BLOCKS,), 1, ROWS + 1), jax.random.fold_in(key_of[1], 1), 1, ROWS).astype(jnp.int32)
    owner_keys = jax.random.split(jax.random.fold_in(key_of[2], 1), BLOCKS // BLK_DEV)
    owner_turns = jax.random.permutation(jax.random.fold_in(key_of[2], 3), BLOCKS // BLK_DEV)
    owner = jax.vmap(lambda own, number: assign_block(jax.random.fold_in(key_of[2], 2), own, number, BLK_DEV, N_GY * N_GZ, 1, 1, 2))(owner_keys, owner_turns).reshape((BLOCKS, 1))
    kdiag = jnp.clip(jnp.exp(math.log(4.0) - 2.0794415 * jax.random.uniform(key_of[3], (SUBDOMAINS, NB), jnp.float32) ** levels(key_of[3], (SUBDOMAINS, NB), ((0, 32),), -0.2, 0.2)), 0.5, 4.0)
    rhs = draw_rhs(jax.random.fold_in(key_of[6], 71), 0)
    modes = noise(key_of[5], (SUBDOMAINS, NC, NB), 1.0, 6.0, ((0, 32),), jnp.float32)
    return dict(blocks=blocks, counts=counts, owner=owner, kdiag=kdiag, rhs=rhs, modes=modes)


def assemble(values):
    count = values.shape[1]
    width = values.shape[2]
    face = width // 8
    grid = values.reshape(N_GX, N_GY, N_GZ, count, width)
    next_x = jnp.roll(grid, -1, axis=0)
    prev_x = jnp.roll(grid, 1, axis=0)
    next_y = jnp.roll(grid, -1, axis=1)
    prev_y = jnp.roll(grid, 1, axis=1)
    next_z = jnp.roll(grid, -1, axis=2)
    prev_z = jnp.roll(grid, 1, axis=2)
    extra = jnp.concatenate([next_x[..., face:2 * face], prev_x[..., 0:face], next_y[..., 3 * face:4 * face], prev_y[..., 2 * face:3 * face], next_z[..., 6 * face:8 * face], prev_z[..., 4 * face:6 * face]], axis=-1)
    return (grid + extra).reshape(values.shape)

def reference(blocks, counts, owner, kdiag, rhs, modes):
    hi = lax.Precision.HIGHEST
    rowid = jnp.arange(ROWS, dtype=jnp.int32)[None, :, None]
    live = jnp.where(rowid < counts[:, None, None], blocks, jnp.zeros_like(blocks)).astype(jnp.float32)
    group = N_GY * N_GZ
    reader = jnp.arange(BLOCKS, dtype=jnp.int32) // BLK_DEV
    target = (reader // group * group + owner[:, 0]).astype(jnp.int32)
    start = jnp.eye(NB, dtype=jnp.float32)[None, :, :] * kdiag[:, :, None]

    def add_block(total, item):
        piece, where = item
        gram = jnp.dot(piece.T, piece, precision=hi)
        return (total.at[where].add(gram), None)
    stiff, _ = lax.scan(add_block, start, (live, target))
    schur = stiff.astype(jnp.bfloat16)
    loaded = assemble(jnp.concatenate([rhs[:, None, :], modes], axis=1))
    force = loaded[:, 0]
    basis = loaded[:, 1:]
    coarse = 0.5 * jnp.einsum('dcn,den->ce', basis, basis, precision=hi)
    gforce = 0.5 * jnp.einsum('dcn,dn->c', basis, force, precision=hi)
    fnorm = 0.5 * jnp.sum(force * force)
    factor = jnp.linalg.cholesky(coarse)
    coef = jax.scipy.linalg.cho_solve((factor, True), gforce)
    residual = force - jnp.einsum('c,dcn->dn', coef, basis, precision=hi)
    norm_now = fnorm - jnp.dot(gforce, coef, precision=hi)
    direction = residual
    solution = jnp.zeros_like(force)
    for step in range(ITERS):
        local = jnp.einsum('dij,dj->di', stiff, direction, precision=hi)
        image = assemble(local[:, None, :])[:, 0]
        gimage = 0.5 * jnp.einsum('dcn,dn->c', basis, image, precision=hi)
        coef = jax.scipy.linalg.cho_solve((factor, True), gimage)
        along = image - jnp.einsum('c,dcn->dn', coef, basis, precision=hi)
        alpha = norm_now / (0.5 * jnp.sum(direction * along))
        solution = solution + alpha * direction
        residual = residual - alpha * along
        norm_next = 0.5 * jnp.sum(residual * residual)
        direction = residual + norm_next / norm_now * direction
        norm_now = norm_next
    return (schur, solution, residual)
```

```python
import functools

import jax
import jax.numpy as jnp
from jax import lax
from jax.experimental import pallas as pl
from jax.experimental.pallas import tpu as pltpu
from jax.sharding import PartitionSpec as P

MESH = pl.DeviceIdType.MESH
HI = lax.Precision.HIGHEST
F32 = jnp.float32
BF16 = jnp.bfloat16
EARLY = 8


def kernel(
    nx, ny, nz,
    counts_ref, owner_ref, blocks_ref, kdiag_ref, rhs_ref, modes_ref,
    schur_ref, sol_ref, res_ref,
    blk, outgoing, arrived, stiff, high, low, stack, ext0, loc, ext, slots,
    load_sem, schur_sem, bsend, brecv, fsend, frecv, rsend, rrecv,
):
    n = nx * ny * nz
    owners = ny * nz
    half = nz // 2
    nblk, nrows, width = blk.shape
    nc = modes_ref.shape[1]
    face = width // 8
    ix, iy, iz = lax.axis_index("gx"), lax.axis_index("gy"), lax.axis_index("gz")
    me = (ix * ny + iy) * nz + iz
    place = iy * nz + iz

    def coords(flat):
        return (flat // (ny * nz), (flat // nz) % ny, flat % nz)

    load = pltpu.make_async_copy(blocks_ref, blk, load_sem)
    load.start()
    barrier = pltpu.get_barrier_semaphore()

    def greet(k, carry):
        pl.semaphore_signal(barrier, inc=1, device_id=coords((me + k) % n), device_id_type=MESH)
        return carry

    lax.fori_loop(1, n, greet, 0)
    stack[...] = jnp.zeros_like(stack)
    stack[0:nc, :] = modes_ref[0]
    stack[nc : nc + 1, :] = rhs_ref[...]
    pl.semaphore_wait(barrier, n - 1)

    next_x, prev_x = ((ix + 1) % nx, iy, iz), ((ix + nx - 1) % nx, iy, iz)
    next_y, prev_y = (ix, (iy + 1) % ny, iz), (ix, (iy + ny - 1) % ny, iz)
    next_z, prev_z = (ix, iy, (iz + 1) % nz), (ix, iy, (iz + nz - 1) % nz)
    plan = (
        (0, 1, 1, next_x), (1, 0, 1, prev_x),
        (2, 3, 1, next_y), (3, 2, 1, prev_y),
        (4, 6, 2, next_z), (6, 4, 2, prev_z),
    )

    def faces(src, dst, turn):
        copies = []
        for at, (mine, theirs, wide, device) in enumerate(plan):
            copies.append(
                pltpu.make_async_remote_copy(
                    src_ref=src.at[:, mine * face : (mine + wide) * face],
                    dst_ref=dst.at[:, theirs * face : (theirs + wide) * face],
                    send_sem=fsend.at[turn, at],
                    recv_sem=frecv.at[turn, at],
                    device_id=device,
                    device_id_type=MESH,
                )
            )
        return copies

    def start_all(copies):
        for copy in copies:
            copy.start()

    def share(turn, row):
        slots[turn, me] = row

        def send(k, carry):
            pltpu.make_async_remote_copy(
                src_ref=slots.at[turn, me],
                dst_ref=slots.at[turn, me],
                send_sem=rsend.at[turn, k],
                recv_sem=rrecv.at[turn, me],
                device_id=coords((me + k) % n),
                device_id_type=MESH,
            ).start()
            return carry

        lax.fori_loop(1, n, send, 0)

    def row_copy(turn, k, src):
        return pltpu.make_async_remote_copy(
            src_ref=slots.at[turn, me],
            dst_ref=slots.at[turn, src],
            send_sem=rsend.at[turn, k],
            recv_sem=rrecv.at[turn, src],
            device_id=coords((me + k) % n),
            device_id_type=MESH,
        )

    def gathered(turn):
        def arrive(k, carry):
            row_copy(turn, k, (me + k) % n).wait_recv()
            return carry

        lax.fori_loop(1, n, arrive, 0)
        return jnp.sum(slots[turn], axis=0)

    def finish_share(turn):
        def sent(k, carry):
            row_copy(turn, k, me).wait_send()
            return carry

        lax.fori_loop(1, n, sent, 0)

    first = faces(stack, ext0, 0)
    start_all(first)
    load.wait()

    owned = [owner_ref[b, 0] for b in range(nblk)]
    counted = [counts_ref[b] for b in range(nblk)]
    rowid = lax.broadcasted_iota(jnp.int32, (nrows, width), 0)

    def chosen(target):
        which = jnp.int32(0)
        count = jnp.int32(0)
        for b in range(nblk):
            same = owned[b] == target
            which = jnp.where(same, b, which)
            count = jnp.where(same, counted[b], count)
        value = blk[which]
        return jnp.where(rowid < count, value, jnp.zeros_like(value))

    def route(t):
        dj = half - 1 - t // (2 * ny)
        dy = ny - 1 - (t % (2 * ny)) // 2
        e = 1 - t % 2
        ty = (iy + dy) % ny
        tz = 2 * ((iz // 2 + dj) % half) + (iz + e) % 2
        return ty, tz

    def block_copy(t, src):
        ty, tz = route(t)
        return pltpu.make_async_remote_copy(
            src_ref=outgoing.at[t],
            dst_ref=arrived.at[pl.ds(pl.multiple_of(src * nrows, nrows), nrows), :],
            send_sem=bsend.at[t],
            recv_sem=brecv.at[src],
            device_id=(ix, ty, tz),
            device_id_type=MESH,
        )

    def push(t, carry):
        ty, tz = route(t)
        outgoing[t] = chosen(ty * nz + tz)
        block_copy(t, place).start()
        return carry

    early = min(EARLY, owners - 1)
    lax.fori_loop(0, early, push, 0)

    lane = lax.broadcasted_iota(jnp.int32, (8, 128), 1)
    sub = lax.broadcasted_iota(jnp.int32, (8, 128), 0)
    sub1 = lax.broadcasted_iota(jnp.int32, (8, 1), 0)
    lane1 = lax.broadcasted_iota(jnp.int32, (1, 128), 1)

    for copy in first:
        copy.wait_recv()
    work = stack[...] + ext0[...]
    tall = jnp.concatenate([work] * 16, axis=0)
    pairs = 0.5 * lax.dot_general(
        work, tall, (((1,), (1,)), ((), ())), precision=HI, preferred_element_type=F32
    )
    share(0, jnp.sum(jnp.where(lane // 8 == sub, pairs, 0.0), axis=0, keepdims=True))
    lax.fori_loop(early, owners - 1, push, 0)
    arrived[pl.ds(pl.multiple_of(place * nrows, nrows), nrows), :] = chosen(place)

    tile = 128
    diag_r = lax.broadcasted_iota(jnp.int32, (tile, width), 0)
    diag_c = lax.broadcasted_iota(jnp.int32, (tile, width), 1)
    for r in range(width // tile):
        stiff[r * tile : (r + 1) * tile, :] = jnp.where(
            diag_r + r * tile == diag_c, kdiag_ref[...], 0.0
        )

    def take(u, carry):
        dj = u // ny
        dy = ny - 1 - u % ny
        sy = (iy + ny - dy) % ny
        sj = (iz // 2 + half - dj) % half
        base = sy * nz + 2 * sj
        for e in range(2):
            src = base + e

            @pl.when(src != place)
            def _():
                block_copy(0, src).wait_recv()

        rows = arrived[pl.ds(pl.multiple_of(base * nrows, 2 * nrows), 2 * nrows), :]
        for c in range(width // 256):
            cols = slice(c * 256, (c + 1) * 256)
            stiff[:, cols] += lax.dot_general(
                rows, rows[:, cols], (((0,), (0,)), ((), ())), preferred_element_type=F32
            )
        return carry

    turns = owners // 2
    lax.fori_loop(0, ny, take, 0)

    total = gathered(0)
    spread = jnp.where(lane // 8 == sub, total, 0.0)
    fold_r = lax.broadcasted_iota(jnp.int32, (128, 128), 0)
    fold_c = lax.broadcasted_iota(jnp.int32, (128, 128), 1)
    fold = jnp.where(fold_r % 8 == fold_c, 1.0, 0.0).astype(F32)
    coarse = jnp.dot(spread, fold, precision=HI, preferred_element_type=F32)
    for k in range(nc):
        ratio = jnp.where(sub1 > k, coarse[:, k : k + 1] / coarse[k : k + 1, k : k + 1], 0.0)
        coarse_row = coarse[k : k + 1, :]
        work_row = work[k : k + 1, :]
        coarse = coarse - ratio * coarse_row
        work = work - ratio * work_row
    diag = jnp.sum(jnp.where(lane == sub, coarse, 0.0), axis=1, keepdims=True)
    norm_now = diag[nc : nc + 1, :]
    work = work * jnp.where(sub1 < nc, 1.0 / jnp.sqrt(jnp.where(sub1 < nc, diag, 1.0)), 1.0)
    direction = work[nc : nc + 1, :]
    basis = jnp.where(sub1 < nc, work, 0.0)

    lax.fori_loop(ny, turns, take, 0)

    for r in range(width // tile):
        rows = slice(r * tile, (r + 1) * tile)
        value = stiff[rows, :]
        top = value.astype(BF16)
        high[rows, :] = top
        low[rows, :] = (value - top.astype(F32)).astype(BF16)
    store = pltpu.make_async_copy(high, schur_ref.at[0], schur_sem)
    store.start()

    sub16 = lax.broadcasted_iota(jnp.int32, (16, width), 0)

    def apply(vector):
        a = vector.astype(BF16).astype(F32)
        b = (vector - a).astype(BF16).astype(F32)
        c = vector - a - b
        left = jnp.where(
            sub16 == 0, a, jnp.where(sub16 == 1, b, jnp.where(sub16 == 2, c, 0.0))
        ).astype(BF16)
        both = jnp.dot(left, high[...], preferred_element_type=F32) + jnp.dot(
            left, low[...], preferred_element_type=F32
        )
        return jnp.sum(both, axis=0, keepdims=True)

    def as_row(column):
        return jnp.sum(jnp.where(lane == sub, column, 0.0), axis=0, keepdims=True)

    def as_column(row):
        return jnp.sum(jnp.where(lane == sub, row, 0.0), axis=1, keepdims=True)

    local = apply(direction)
    loc[0] = local
    second = faces(loc.at[0], ext.at[0], 1)
    start_all(second)
    share(1, as_row(jnp.sum(work * local, axis=1, keepdims=True)))
    for copy in second:
        copy.wait_recv()
    image = local + ext[0]
    g_one = as_column(gathered(1))
    curve_one = g_one[nc : nc + 1, :]
    alpha = norm_now / curve_one
    along = image - jnp.sum(g_one * basis, axis=0, keepdims=True)
    residual = direction - alpha * along
    answer = alpha * direction

    local = apply(residual)
    loc[1] = local
    third = faces(loc.at[1], ext.at[1], 2)
    start_all(third)
    probe = jnp.where(sub1 == nc + 1, residual, work)
    square = 0.5 * jnp.sum(residual * residual, axis=1, keepdims=True)
    row = as_row(jnp.sum(probe * local, axis=1, keepdims=True))
    share(2, jnp.where(lane1 == 8, square, row))
    for copy in third:
        copy.wait_recv()
    total = gathered(2)
    g_two = as_column(total)
    norm_next = jnp.sum(jnp.where(lane1 == 8, total, 0.0), axis=1, keepdims=True)
    beta = norm_next / norm_now
    curve = (
        g_two[nc + 1 : nc + 2, :]
        + 2.0 * beta * g_two[nc : nc + 1, :]
        + beta * beta * curve_one
    )
    image = local + ext[1] + beta * image
    along = image - jnp.sum((g_two + beta * g_one) * basis, axis=0, keepdims=True)
    alpha = norm_next / curve
    sol_ref[...] = answer + alpha * (residual + beta * direction)
    res_ref[...] = residual - alpha * along

    for copies in (first, second, third):
        for copy in copies:
            copy.wait_send()
    for turn in range(3):
        finish_share(turn)

    def drained(t, carry):
        block_copy(t, place).wait_send()
        return carry

    lax.fori_loop(0, owners - 1, drained, 0)
    store.wait()


def solution(mesh):
    nx, ny, nz = mesh.shape["gx"], mesh.shape["gy"], mesh.shape["gz"]
    n, owners = nx * ny * nz, ny * nz

    def shards(blocks, counts, owner, kdiag, rhs, modes):
        nblk, nrows, width = blocks.shape
        vmem = pl.BlockSpec(memory_space=pltpu.VMEM)
        smem = pl.BlockSpec(memory_space=pltpu.SMEM)
        hbm = pl.BlockSpec(memory_space=pl.ANY)
        return pl.pallas_call(
            functools.partial(kernel, nx, ny, nz),
            out_shape=(
                jax.ShapeDtypeStruct((1, width, width), BF16),
                jax.ShapeDtypeStruct((1, width), F32),
                jax.ShapeDtypeStruct((1, width), F32),
            ),
            in_specs=[smem, smem, hbm, vmem, vmem, vmem],
            out_specs=(hbm, vmem, vmem),
            scratch_shapes=[
                pltpu.VMEM((nblk, nrows, width), BF16),
                pltpu.VMEM((owners, nrows, width), BF16),
                pltpu.VMEM((owners * nrows, width), BF16),
                pltpu.VMEM((width, width), F32),
                pltpu.VMEM((width, width), BF16),
                pltpu.VMEM((width, width), BF16),
                pltpu.VMEM((8, width), F32),
                pltpu.VMEM((8, width), F32),
                pltpu.VMEM((2, 1, width), F32),
                pltpu.VMEM((2, 1, width), F32),
                pltpu.VMEM((3, n, 1, 128), F32),
                pltpu.SemaphoreType.DMA,
                pltpu.SemaphoreType.DMA,
                pltpu.SemaphoreType.DMA((owners,)),
                pltpu.SemaphoreType.DMA((owners,)),
                pltpu.SemaphoreType.DMA((3, 6)),
                pltpu.SemaphoreType.DMA((3, 6)),
                pltpu.SemaphoreType.DMA((3, n)),
                pltpu.SemaphoreType.DMA((3, n)),
            ],
            compiler_params=pltpu.CompilerParams(
                collective_id=0, has_side_effects=True, vmem_limit_bytes=60000 * 1024
            ),
        )(counts, owner, blocks, kdiag, rhs, modes)

    every = ("gx", "gy", "gz")
    return jax.shard_map(
        shards,
        mesh=mesh,
        in_specs=(
            P(every, None, None), P(every), P(every, None),
            P(every, None), P(every, None), P(every, None, None),
        ),
        out_specs=(P(every, None, None), P(every, None), P(every, None)),
        check_vma=False,
    )
```

```python
import functools

import jax
import jax.numpy as jnp
from jax import lax
from jax.experimental import pallas as pl
from jax.experimental.pallas import tpu as pltpu
from jax.sharding import PartitionSpec as P

MESH = pl.DeviceIdType.MESH
HI = lax.Precision.HIGHEST
F32 = jnp.float32
BF16 = jnp.bfloat16
EARLY = 8


def kernel(
    nx, ny, nz,
    counts_ref, owner_ref, blocks_ref, kdiag_ref, rhs_ref, modes_ref,
    schur_ref, sol_ref, res_ref,
    blk, outgoing, arrived, stiff, high, low, stack, ext0, loc, ext, slots,
    load_sem, schur_sem, bsend, brecv, fsend, frecv, rsend, rrecv,
):
    n = nx * ny * nz
    owners = ny * nz
    half = nz // 2
    nblk, nrows, width = blk.shape
    nc = modes_ref.shape[0]
    face = width // 8
    ix, iy, iz = lax.axis_index("gx"), lax.axis_index("gy"), lax.axis_index("gz")
    me = (ix * ny + iy) * nz + iz
    place = iy * nz + iz
    outer = jnp.logical_or(iz == 0, iz == nz - 1)

    def coords(flat):
        return (flat // (ny * nz), (flat // nz) % ny, flat % nz)

    load = pltpu.make_async_copy(blocks_ref, blk, load_sem)
    load.start()
    barrier = pltpu.get_barrier_semaphore()

    def greet(k, carry):
        pl.semaphore_signal(barrier, inc=1, device_id=coords((me + k) % n), device_id_type=MESH)
        return carry

    lax.fori_loop(1, n, greet, 0)
    stack[...] = jnp.zeros_like(stack)
    for i in range(nc):
        stack[i : i + 1, :] = modes_ref[i]
    stack[nc : nc + 1, :] = rhs_ref[...]
    pl.semaphore_wait(barrier, n - 1)

    next_x, prev_x = ((ix + 1) % nx, iy, iz), ((ix + nx - 1) % nx, iy, iz)
    next_y, prev_y = (ix, (iy + 1) % ny, iz), (ix, (iy + ny - 1) % ny, iz)
    next_z, prev_z = (ix, iy, (iz + 1) % nz), (ix, iy, (iz + nz - 1) % nz)
    plan = (
        (0, 1, 1, next_x), (1, 0, 1, prev_x),
        (2, 3, 1, next_y), (3, 2, 1, prev_y),
        (4, 6, 2, next_z), (6, 4, 2, prev_z),
    )

    def faces(src, dst, turn):
        copies = []
        for at, (mine, theirs, wide, device) in enumerate(plan):
            copies.append(
                pltpu.make_async_remote_copy(
                    src_ref=src.at[:, mine * face : (mine + wide) * face],
                    dst_ref=dst.at[:, theirs * face : (theirs + wide) * face],
                    send_sem=fsend.at[turn, at],
                    recv_sem=frecv.at[turn, at],
                    device_id=device,
                    device_id_type=MESH,
                )
            )
        return copies

    def start_all(copies):
        for copy in copies:
            copy.start()

    def share(turn, row):
        slots[turn, me] = row

        def send(k, carry):
            pltpu.make_async_remote_copy(
                src_ref=slots.at[turn, me],
                dst_ref=slots.at[turn, me],
                send_sem=rsend.at[turn, k],
                recv_sem=rrecv.at[turn, me],
                device_id=coords((me + k) % n),
                device_id_type=MESH,
            ).start()
            return carry

        lax.fori_loop(1, n, send, 0)

    def row_copy(turn, k, src):
        return pltpu.make_async_remote_copy(
            src_ref=slots.at[turn, me],
            dst_ref=slots.at[turn, src],
            send_sem=rsend.at[turn, k],
            recv_sem=rrecv.at[turn, src],
            device_id=coords((me + k) % n),
            device_id_type=MESH,
        )

    def gathered(turn):
        def arrive(k, carry):
            row_copy(turn, k, (me + k) % n).wait_recv()
            return carry

        lax.fori_loop(1, n, arrive, 0)
        return jnp.sum(slots[turn], axis=0)

    def finish_share(turn):
        def sent(k, carry):
            row_copy(turn, k, me).wait_send()
            return carry

        lax.fori_loop(1, n, sent, 0)

    first = faces(stack, ext0, 0)
    start_all(first)
    load.wait()

    owned = [owner_ref[b] for b in range(nblk)]
    counted = [counts_ref[b] for b in range(nblk)]
    rowid = lax.broadcasted_iota(jnp.int32, (nrows, width), 0)

    def chosen(target):
        which = jnp.int32(0)
        count = jnp.int32(0)
        for b in range(nblk):
            same = owned[b] == target
            which = jnp.where(same, b, which)
            count = jnp.where(same, counted[b], count)
        value = blk[which]
        return jnp.where(rowid < count, value, jnp.zeros_like(value))

    def route(t):
        far = owners - 2 * ny
        inner = jnp.where(t < far, t + 2 * ny, t - far + 1)
        order = jnp.where(outer, t + 1, inner)
        dj = order // (2 * ny)
        dy = (order % (2 * ny)) // 2
        e = order % 2
        ty = (iy + dy) % ny
        tz = 2 * ((iz // 2 + dj) % half) + (iz + e) % 2
        return ty, tz

    def block_copy(t, src):
        ty, tz = route(t)
        return pltpu.make_async_remote_copy(
            src_ref=outgoing.at[t],
            dst_ref=arrived.at[pl.ds(pl.multiple_of(src * nrows, nrows), nrows), :],
            send_sem=bsend.at[t],
            recv_sem=brecv.at[src],
            device_id=(ix, ty, tz),
            device_id_type=MESH,
        )

    def push(t, carry):
        ty, tz = route(t)
        outgoing[t] = chosen(ty * nz + tz)
        block_copy(t, place).start()
        return carry

    early = min(EARLY, owners - 1)
    lax.fori_loop(0, early, push, 0)

    lane = lax.broadcasted_iota(jnp.int32, (8, 128), 1)
    sub = lax.broadcasted_iota(jnp.int32, (8, 128), 0)
    sub1 = lax.broadcasted_iota(jnp.int32, (8, 1), 0)
    lane1 = lax.broadcasted_iota(jnp.int32, (1, 128), 1)

    for copy in first:
        copy.wait_recv()
    work = stack[...] + ext0[...]
    tall = jnp.concatenate([work] * 16, axis=0)
    pairs = 0.5 * lax.dot_general(
        work, tall, (((1,), (1,)), ((), ())), precision=HI, preferred_element_type=F32
    )
    share(0, jnp.sum(jnp.where(lane // 8 == sub, pairs, 0.0), axis=0, keepdims=True))
    lax.fori_loop(early, owners - 1, push, 0)
    arrived[pl.ds(pl.multiple_of(place * nrows, nrows), nrows), :] = chosen(place)

    tile = 128
    diag_r = lax.broadcasted_iota(jnp.int32, (tile, width), 0)
    diag_c = lax.broadcasted_iota(jnp.int32, (tile, width), 1)
    for r in range(width // tile):
        stiff[r * tile : (r + 1) * tile, :] = jnp.where(
            diag_r + r * tile == diag_c, kdiag_ref[...], 0.0
        )

    def take(u, carry):
        dj = u // ny
        dy = u % ny
        sy = (iy + ny - dy) % ny
        sj = (iz // 2 + half - dj) % half
        base = sy * nz + 2 * sj
        for e in range(2):
            src = base + e

            @pl.when(src != place)
            def _():
                block_copy(0, src).wait_recv()

        rows = arrived[pl.ds(pl.multiple_of(base * nrows, 2 * nrows), 2 * nrows), :]
        for c in range(width // 256):
            cols = slice(c * 256, (c + 1) * 256)
            stiff[:, cols] += lax.dot_general(
                rows, rows[:, cols], (((0,), (0,)), ((), ())), preferred_element_type=F32
            )
        return carry

    turns = owners // 2
    lax.fori_loop(0, ny, take, 0)

    total = gathered(0)
    spread = jnp.where(lane // 8 == sub, total, 0.0)
    fold_r = lax.broadcasted_iota(jnp.int32, (128, 128), 0)
    fold_c = lax.broadcasted_iota(jnp.int32, (128, 128), 1)
    fold = jnp.where(fold_r % 8 == fold_c, 1.0, 0.0).astype(F32)
    coarse = jnp.dot(spread, fold, precision=HI, preferred_element_type=F32)
    for k in range(nc):
        ratio = jnp.where(sub1 > k, coarse[:, k : k + 1] / coarse[k : k + 1, k : k + 1], 0.0)
        coarse_row = coarse[k : k + 1, :]
        work_row = work[k : k + 1, :]
        coarse = coarse - ratio * coarse_row
        work = work - ratio * work_row
    diag = jnp.sum(jnp.where(lane == sub, coarse, 0.0), axis=1, keepdims=True)
    norm_now = diag[nc : nc + 1, :]
    work = work * jnp.where(sub1 < nc, 1.0 / jnp.sqrt(jnp.where(sub1 < nc, diag, 1.0)), 1.0)
    direction = work[nc : nc + 1, :]
    basis = jnp.where(sub1 < nc, work, 0.0)

    lax.fori_loop(ny, turns, take, 0)

    for r in range(width // tile):
        rows = slice(r * tile, (r + 1) * tile)
        value = stiff[rows, :]
        top = value.astype(BF16)
        high[rows, :] = top
        low[rows, :] = (value - top.astype(F32)).astype(BF16)
    store = pltpu.make_async_copy(high, schur_ref.at[0], schur_sem)
    store.start()

    sub16 = lax.broadcasted_iota(jnp.int32, (16, width), 0)

    def apply(vector):
        a = vector.astype(BF16).astype(F32)
        b = (vector - a).astype(BF16).astype(F32)
        c = vector - a - b
        left = jnp.where(
            sub16 == 0, a, jnp.where(sub16 == 1, b, jnp.where(sub16 == 2, c, 0.0))
        ).astype(BF16)
        both = jnp.dot(left, high[...], preferred_element_type=F32) + jnp.dot(
            left, low[...], preferred_element_type=F32
        )
        return jnp.sum(both, axis=0, keepdims=True)

    def as_row(column):
        return jnp.sum(jnp.where(lane == sub, column, 0.0), axis=0, keepdims=True)

    def as_column(row):
        return jnp.sum(jnp.where(lane == sub, row, 0.0), axis=1, keepdims=True)

    local = apply(direction)
    loc[0] = local
    second = faces(loc.at[0], ext.at[0], 1)
    start_all(second)
    share(1, as_row(jnp.sum(work * local, axis=1, keepdims=True)))
    for copy in second:
        copy.wait_recv()
    image = local + ext[0]
    g_one = as_column(gathered(1))
    curve_one = g_one[nc : nc + 1, :]
    alpha = norm_now / curve_one
    along = image - jnp.sum(g_one * basis, axis=0, keepdims=True)
    residual = direction - alpha * along
    answer = alpha * direction

    local = apply(residual)
    loc[1] = local
    third = faces(loc.at[1], ext.at[1], 2)
    start_all(third)
    probe = jnp.where(sub1 == nc + 1, residual, work)
    square = 0.5 * jnp.sum(residual * residual, axis=1, keepdims=True)
    row = as_row(jnp.sum(probe * local, axis=1, keepdims=True))
    share(2, jnp.where(lane1 == 8, square, row))
    for copy in third:
        copy.wait_recv()
    total = gathered(2)
    g_two = as_column(total)
    norm_next = jnp.sum(jnp.where(lane1 == 8, total, 0.0), axis=1, keepdims=True)
    beta = norm_next / norm_now
    curve = (
        g_two[nc + 1 : nc + 2, :]
        + 2.0 * beta * g_two[nc : nc + 1, :]
        + beta * beta * curve_one
    )
    image = local + ext[1] + beta * image
    along = image - jnp.sum((g_two + beta * g_one) * basis, axis=0, keepdims=True)
    alpha = norm_next / curve
    sol_ref[...] = answer + alpha * (residual + beta * direction)
    res_ref[...] = residual - alpha * along

    for copies in (first, second, third):
        for copy in copies:
            copy.wait_send()
    for turn in range(3):
        finish_share(turn)

    def drained(t, carry):
        block_copy(t, place).wait_send()
        return carry

    lax.fori_loop(0, owners - 1, drained, 0)
    store.wait()


def finish(schur_in, sol_in, res_in, schur_ref, sol_ref, res_ref, held, in_sem, out_sem):
    parts = held.shape[0]
    rows = held.shape[1]
    loads, stores = [], []
    for i in range(parts):
        span = pl.ds(i * rows, rows)
        loads.append(pltpu.make_async_copy(schur_in.at[0, span], held.at[i], in_sem.at[i]))
        stores.append(pltpu.make_async_copy(held.at[i], schur_ref.at[0, span], out_sem.at[i]))
    for load in loads:
        load.start()
    sol_ref[...] = sol_in[...]
    res_ref[...] = res_in[...]
    for load, store in zip(loads, stores):
        load.wait()
        store.start()
    for store in stores:
        store.wait()


def solution(mesh):
    nx, ny, nz = mesh.shape["gx"], mesh.shape["gy"], mesh.shape["gz"]
    n, owners = nx * ny * nz, ny * nz

    def shards(blocks, counts, owner, kdiag, rhs, modes):
        nblk, nrows, width = blocks.shape
        vmem = pl.BlockSpec(memory_space=pltpu.VMEM)
        smem = pl.BlockSpec(memory_space=pltpu.SMEM)
        hbm = pl.BlockSpec(memory_space=pl.ANY)
        made = pl.pallas_call(
            functools.partial(kernel, nx, ny, nz),
            out_shape=(
                jax.ShapeDtypeStruct((1, width, width), BF16),
                jax.ShapeDtypeStruct((1, width), F32),
                jax.ShapeDtypeStruct((1, width), F32),
            ),
            in_specs=[smem, smem, hbm, vmem, vmem, vmem],
            out_specs=(hbm, vmem, vmem),
            scratch_shapes=[
                pltpu.VMEM((nblk, nrows, width), BF16),
                pltpu.VMEM((owners, nrows, width), BF16),
                pltpu.VMEM((owners * nrows, width), BF16),
                pltpu.VMEM((width, width), F32),
                pltpu.VMEM((width, width), BF16),
                pltpu.VMEM((width, width), BF16),
                pltpu.VMEM((8, width), F32),
                pltpu.VMEM((8, width), F32),
                pltpu.VMEM((2, 1, width), F32),
                pltpu.VMEM((2, 1, width), F32),
                pltpu.VMEM((3, n, 1, 128), F32),
                pltpu.SemaphoreType.DMA,
                pltpu.SemaphoreType.DMA,
                pltpu.SemaphoreType.DMA((owners,)),
                pltpu.SemaphoreType.DMA((owners,)),
                pltpu.SemaphoreType.DMA((3, 6)),
                pltpu.SemaphoreType.DMA((3, 6)),
                pltpu.SemaphoreType.DMA((3, n)),
                pltpu.SemaphoreType.DMA((3, n)),
            ],
            compiler_params=pltpu.CompilerParams(
                collective_id=0, has_side_effects=True, vmem_limit_bytes=60000 * 1024
            ),
        )(counts, owner[:, 0], blocks, kdiag, rhs, jnp.transpose(modes, (1, 0, 2)))
        return pl.pallas_call(
            finish,
            out_shape=(
                jax.ShapeDtypeStruct((1, width, width), BF16),
                jax.ShapeDtypeStruct((1, width), F32),
                jax.ShapeDtypeStruct((1, width), F32),
            ),
            in_specs=[hbm, vmem, vmem],
            out_specs=(hbm, vmem, vmem),
            scratch_shapes=[
                pltpu.VMEM((8, width // 8, width), BF16),
                pltpu.SemaphoreType.DMA((8,)),
                pltpu.SemaphoreType.DMA((8,)),
            ],
        )(*made)

    every = ("gx", "gy", "gz")
    return jax.shard_map(
        shards,
        mesh=mesh,
        in_specs=(
            P(every, None, None), P(every), P(every, None),
            P(every, None), P(every, None), P(every, None, None),
        ),
        out_specs=(P(every, None, None), P(every, None), P(every, None)),
        check_vma=False,
    )
```

```python
import functools

import jax
import jax.numpy as jnp
from jax import lax
from jax.experimental import pallas as pl
from jax.experimental.pallas import tpu as pltpu
from jax.sharding import PartitionSpec as P

MESH = pl.DeviceIdType.MESH
HI = lax.Precision.HIGHEST
F32 = jnp.float32
BF16 = jnp.bfloat16
EARLY = 8


def kernel(
    nx, ny, nz,
    counts_ref, owner_ref, blocks_ref, kdiag_ref, rhs_ref, modes_ref,
    schur_ref, sol_ref, res_ref,
    blk, outgoing, arrived, stiff, high, low, stack, ext0, loc, ext, slots,
    load_sem, schur_sem, bsend, brecv, fsend, frecv, rsend, rrecv,
):
    n = nx * ny * nz
    owners = ny * nz
    half = nz // 2
    nblk, nrows, width = blk.shape
    nc = modes_ref.shape[0]
    face = width // 8
    ix, iy, iz = lax.axis_index("gx"), lax.axis_index("gy"), lax.axis_index("gz")
    me = (ix * ny + iy) * nz + iz
    place = iy * nz + iz
    outer = jnp.logical_or(iz == 0, iz == nz - 1)

    def coords(flat):
        return (flat // (ny * nz), (flat // nz) % ny, flat % nz)

    load = pltpu.make_async_copy(blocks_ref, blk, load_sem)
    load.start()
    barrier = pltpu.get_barrier_semaphore()

    def greet(k, carry):
        pl.semaphore_signal(barrier, inc=1, device_id=coords((me + k) % n), device_id_type=MESH)
        return carry

    lax.fori_loop(1, n, greet, 0)
    stack[...] = jnp.zeros_like(stack)
    for i in range(nc):
        stack[i : i + 1, :] = modes_ref[i]
    stack[nc : nc + 1, :] = rhs_ref[...]
    pl.semaphore_wait(barrier, n - 1)

    next_x, prev_x = ((ix + 1) % nx, iy, iz), ((ix + nx - 1) % nx, iy, iz)
    next_y, prev_y = (ix, (iy + 1) % ny, iz), (ix, (iy + ny - 1) % ny, iz)
    next_z, prev_z = (ix, iy, (iz + 1) % nz), (ix, iy, (iz + nz - 1) % nz)
    plan = (
        (0, 1, 1, next_x), (1, 0, 1, prev_x),
        (2, 3, 1, next_y), (3, 2, 1, prev_y),
        (4, 6, 2, next_z), (6, 4, 2, prev_z),
    )

    def faces(src, dst, turn):
        copies = []
        for at, (mine, theirs, wide, device) in enumerate(plan):
            copies.append(
                pltpu.make_async_remote_copy(
                    src_ref=src.at[:, mine * face : (mine + wide) * face],
                    dst_ref=dst.at[:, theirs * face : (theirs + wide) * face],
                    send_sem=fsend.at[turn, at],
                    recv_sem=frecv.at[turn, at],
                    device_id=device,
                    device_id_type=MESH,
                )
            )
        return copies

    def start_all(copies):
        for copy in copies:
            copy.start()

    def share(turn, row):
        slots[turn, me] = row

        def send(k, carry):
            pltpu.make_async_remote_copy(
                src_ref=slots.at[turn, me],
                dst_ref=slots.at[turn, me],
                send_sem=rsend.at[turn, k],
                recv_sem=rrecv.at[turn, me],
                device_id=coords((me + k) % n),
                device_id_type=MESH,
            ).start()
            return carry

        lax.fori_loop(1, n, send, 0)

    def row_copy(turn, k, src):
        return pltpu.make_async_remote_copy(
            src_ref=slots.at[turn, me],
            dst_ref=slots.at[turn, src],
            send_sem=rsend.at[turn, k],
            recv_sem=rrecv.at[turn, src],
            device_id=coords((me + k) % n),
            device_id_type=MESH,
        )

    def gathered(turn):
        def arrive(k, carry):
            row_copy(turn, k, (me + k) % n).wait_recv()
            return carry

        lax.fori_loop(1, n, arrive, 0)
        return jnp.sum(slots[turn], axis=0)

    def finish_share(turn):
        def sent(k, carry):
            row_copy(turn, k, me).wait_send()
            return carry

        lax.fori_loop(1, n, sent, 0)

    first = faces(stack, ext0, 0)
    start_all(first)
    load.wait()

    owned = [owner_ref[b] for b in range(nblk)]
    counted = [counts_ref[b] for b in range(nblk)]
    rowid = lax.broadcasted_iota(jnp.int32, (nrows, width), 0)

    def chosen(target):
        which = jnp.int32(0)
        count = jnp.int32(0)
        for b in range(nblk):
            same = owned[b] == target
            which = jnp.where(same, b, which)
            count = jnp.where(same, counted[b], count)
        value = blk[which]
        return jnp.where(rowid < count, value, jnp.zeros_like(value))

    def route(t):
        far = owners - 2 * ny
        inner = jnp.where(t < far, t + 2 * ny, t - far + 1)
        order = jnp.where(outer, t + 1, jnp.where(t % 2 == 0, 2 * ny + t // 2, t // 2 + 1))
        dj = order // (2 * ny)
        dy = (order % (2 * ny)) // 2
        e = order % 2
        ty = (iy + dy) % ny
        tz = 2 * ((iz // 2 + dj) % half) + (iz + e) % 2
        return ty, tz

    def block_copy(t, src):
        ty, tz = route(t)
        return pltpu.make_async_remote_copy(
            src_ref=outgoing.at[t],
            dst_ref=arrived.at[pl.ds(pl.multiple_of(src * nrows, nrows), nrows), :],
            send_sem=bsend.at[t],
            recv_sem=brecv.at[src],
            device_id=(ix, ty, tz),
            device_id_type=MESH,
        )

    def push(t, carry):
        ty, tz = route(t)
        outgoing[t] = chosen(ty * nz + tz)
        block_copy(t, place).start()
        return carry

    early = min(EARLY, owners - 1)
    lax.fori_loop(0, early, push, 0)

    lane = lax.broadcasted_iota(jnp.int32, (8, 128), 1)
    sub = lax.broadcasted_iota(jnp.int32, (8, 128), 0)
    sub1 = lax.broadcasted_iota(jnp.int32, (8, 1), 0)
    lane1 = lax.broadcasted_iota(jnp.int32, (1, 128), 1)

    for copy in first:
        copy.wait_recv()
    work = stack[...] + ext0[...]
    tall = jnp.concatenate([work] * 16, axis=0)
    pairs = 0.5 * lax.dot_general(
        work, tall, (((1,), (1,)), ((), ())), precision=HI, preferred_element_type=F32
    )
    share(0, jnp.sum(jnp.where(lane // 8 == sub, pairs, 0.0), axis=0, keepdims=True))
    lax.fori_loop(early, owners - 1, push, 0)
    arrived[pl.ds(pl.multiple_of(place * nrows, nrows), nrows), :] = chosen(place)

    tile = 128
    diag_r = lax.broadcasted_iota(jnp.int32, (tile, width), 0)
    diag_c = lax.broadcasted_iota(jnp.int32, (tile, width), 1)
    for r in range(width // tile):
        stiff[r * tile : (r + 1) * tile, :] = jnp.where(
            diag_r + r * tile == diag_c, kdiag_ref[...], 0.0
        )

    def take(u, carry):
        dj = u // ny
        dy = u % ny
        sy = (iy + ny - dy) % ny
        sj = (iz // 2 + half - dj) % half
        base = sy * nz + 2 * sj
        for e in range(2):
            src = base + e

            @pl.when(src != place)
            def _():
                block_copy(0, src).wait_recv()

        rows = arrived[pl.ds(pl.multiple_of(base * nrows, 2 * nrows), 2 * nrows), :]
        for c in range(width // 256):
            cols = slice(c * 256, (c + 1) * 256)
            stiff[:, cols] += lax.dot_general(
                rows, rows[:, cols], (((0,), (0,)), ((), ())), preferred_element_type=F32
            )
        return carry

    turns = owners // 2
    lax.fori_loop(0, ny, take, 0)

    total = gathered(0)
    spread = jnp.where(lane // 8 == sub, total, 0.0)
    fold_r = lax.broadcasted_iota(jnp.int32, (128, 128), 0)
    fold_c = lax.broadcasted_iota(jnp.int32, (128, 128), 1)
    fold = jnp.where(fold_r % 8 == fold_c, 1.0, 0.0).astype(F32)
    coarse = jnp.dot(spread, fold, precision=HI, preferred_element_type=F32)
    for k in range(nc):
        ratio = jnp.where(sub1 > k, coarse[:, k : k + 1] / coarse[k : k + 1, k : k + 1], 0.0)
        coarse_row = coarse[k : k + 1, :]
        work_row = work[k : k + 1, :]
        coarse = coarse - ratio * coarse_row
        work = work - ratio * work_row
    diag = jnp.sum(jnp.where(lane == sub, coarse, 0.0), axis=1, keepdims=True)
    norm_now = diag[nc : nc + 1, :]
    work = work * jnp.where(sub1 < nc, 1.0 / jnp.sqrt(jnp.where(sub1 < nc, diag, 1.0)), 1.0)
    direction = work[nc : nc + 1, :]
    basis = jnp.where(sub1 < nc, work, 0.0)

    lax.fori_loop(ny, turns, take, 0)

    for r in range(width // tile):
        rows = slice(r * tile, (r + 1) * tile)
        value = stiff[rows, :]
        top = value.astype(BF16)
        high[rows, :] = top
        low[rows, :] = (value - top.astype(F32)).astype(BF16)
    store = pltpu.make_async_copy(high, schur_ref.at[0], schur_sem)
    store.start()

    sub16 = lax.broadcasted_iota(jnp.int32, (16, width), 0)

    def apply(vector):
        a = vector.astype(BF16).astype(F32)
        b = (vector - a).astype(BF16).astype(F32)
        c = vector - a - b
        left = jnp.where(
            sub16 == 0, a, jnp.where(sub16 == 1, b, jnp.where(sub16 == 2, c, 0.0))
        ).astype(BF16)
        both = jnp.dot(left, high[...], preferred_element_type=F32) + jnp.dot(
            left, low[...], preferred_element_type=F32
        )
        return jnp.sum(both, axis=0, keepdims=True)

    def as_row(column):
        return jnp.sum(jnp.where(lane == sub, column, 0.0), axis=0, keepdims=True)

    def as_column(row):
        return jnp.sum(jnp.where(lane == sub, row, 0.0), axis=1, keepdims=True)

    local = apply(direction)
    loc[0] = local
    second = faces(loc.at[0], ext.at[0], 1)
    start_all(second)
    share(1, as_row(jnp.sum(work * local, axis=1, keepdims=True)))
    for copy in second:
        copy.wait_recv()
    image = local + ext[0]
    g_one = as_column(gathered(1))
    curve_one = g_one[nc : nc + 1, :]
    alpha = norm_now / curve_one
    along = image - jnp.sum(g_one * basis, axis=0, keepdims=True)
    residual = direction - alpha * along
    answer = alpha * direction

    local = apply(residual)
    loc[1] = local
    third = faces(loc.at[1], ext.at[1], 2)
    start_all(third)
    probe = jnp.where(sub1 == nc + 1, residual, work)
    square = 0.5 * jnp.sum(residual * residual, axis=1, keepdims=True)
    row = as_row(jnp.sum(probe * local, axis=1, keepdims=True))
    share(2, jnp.where(lane1 == 8, square, row))
    for copy in third:
        copy.wait_recv()
    total = gathered(2)
    g_two = as_column(total)
    norm_next = jnp.sum(jnp.where(lane1 == 8, total, 0.0), axis=1, keepdims=True)
    beta = norm_next / norm_now
    curve = (
        g_two[nc + 1 : nc + 2, :]
        + 2.0 * beta * g_two[nc : nc + 1, :]
        + beta * beta * curve_one
    )
    image = local + ext[1] + beta * image
    along = image - jnp.sum((g_two + beta * g_one) * basis, axis=0, keepdims=True)
    alpha = norm_next / curve
    sol_ref[...] = answer + alpha * (residual + beta * direction)
    res_ref[...] = residual - alpha * along

    for copies in (first, second, third):
        for copy in copies:
            copy.wait_send()
    for turn in range(3):
        finish_share(turn)

    def drained(t, carry):
        block_copy(t, place).wait_send()
        return carry

    lax.fori_loop(0, owners - 1, drained, 0)
    store.wait()


def finish(schur_in, sol_in, res_in, schur_ref, sol_ref, res_ref, held, in_sem, out_sem):
    parts = held.shape[0]
    rows = held.shape[1]
    loads, stores = [], []
    for i in range(parts):
        span = pl.ds(i * rows, rows)
        loads.append(pltpu.make_async_copy(schur_in.at[0, span], held.at[i], in_sem.at[i]))
        stores.append(pltpu.make_async_copy(held.at[i], schur_ref.at[0, span], out_sem.at[i]))
    for load in loads:
        load.start()
    sol_ref[...] = sol_in[...]
    res_ref[...] = res_in[...]
    for load, store in zip(loads, stores):
        load.wait()
        store.start()
    for store in stores:
        store.wait()


def solution(mesh):
    nx, ny, nz = mesh.shape["gx"], mesh.shape["gy"], mesh.shape["gz"]
    n, owners = nx * ny * nz, ny * nz

    def shards(blocks, counts, owner, kdiag, rhs, modes):
        nblk, nrows, width = blocks.shape
        vmem = pl.BlockSpec(memory_space=pltpu.VMEM)
        smem = pl.BlockSpec(memory_space=pltpu.SMEM)
        hbm = pl.BlockSpec(memory_space=pl.ANY)
        made = pl.pallas_call(
            functools.partial(kernel, nx, ny, nz),
            out_shape=(
                jax.ShapeDtypeStruct((1, width, width), BF16),
                jax.ShapeDtypeStruct((1, width), F32),
                jax.ShapeDtypeStruct((1, width), F32),
            ),
            in_specs=[smem, smem, hbm, vmem, vmem, vmem],
            out_specs=(hbm, vmem, vmem),
            scratch_shapes=[
                pltpu.VMEM((nblk, nrows, width), BF16),
                pltpu.VMEM((owners, nrows, width), BF16),
                pltpu.VMEM((owners * nrows, width), BF16),
                pltpu.VMEM((width, width), F32),
                pltpu.VMEM((width, width), BF16),
                pltpu.VMEM((width, width), BF16),
                pltpu.VMEM((8, width), F32),
                pltpu.VMEM((8, width), F32),
                pltpu.VMEM((2, 1, width), F32),
                pltpu.VMEM((2, 1, width), F32),
                pltpu.VMEM((3, n, 1, 128), F32),
                pltpu.SemaphoreType.DMA,
                pltpu.SemaphoreType.DMA,
                pltpu.SemaphoreType.DMA((owners,)),
                pltpu.SemaphoreType.DMA((owners,)),
                pltpu.SemaphoreType.DMA((3, 6)),
                pltpu.SemaphoreType.DMA((3, 6)),
                pltpu.SemaphoreType.DMA((3, n)),
                pltpu.SemaphoreType.DMA((3, n)),
            ],
            compiler_params=pltpu.CompilerParams(
                collective_id=0, has_side_effects=True, vmem_limit_bytes=60000 * 1024
            ),
        )(counts, owner[:, 0], blocks, kdiag, rhs, jnp.transpose(modes, (1, 0, 2)))
        return pl.pallas_call(
            finish,
            out_shape=(
                jax.ShapeDtypeStruct((1, width, width), BF16),
                jax.ShapeDtypeStruct((1, width), F32),
                jax.ShapeDtypeStruct((1, width), F32),
            ),
            in_specs=[hbm, vmem, vmem],
            out_specs=(hbm, vmem, vmem),
            scratch_shapes=[
                pltpu.VMEM((8, width // 8, width), BF16),
                pltpu.SemaphoreType.DMA((8,)),
                pltpu.SemaphoreType.DMA((8,)),
            ],
        )(*made)

    every = ("gx", "gy", "gz")
    return jax.shard_map(
        shards,
        mesh=mesh,
        in_specs=(
            P(every, None, None), P(every), P(every, None),
            P(every, None), P(every, None), P(every, None, None),
        ),
        out_specs=(P(every, None, None), P(every, None), P(every, None)),
        check_vma=False,
    )
```
